32 devices in a mesh: pb: 4 (over z), pa: 8 (over y, x, core).
Axes of the slice: x: 2, y: 2, z: 4, core: 2. Of those that a mesh axis runs over, the one named last changes fastest.
Arguments:
- queries: bfloat16 [4096, 3584], P(('pb', 'pa')), may hold values from -16 to 16
- passages: bfloat16 [16384, 3584], P(('pb', 'pa')), may hold values from -16 to 16
- hard_block_offsets: int32 [1024, 4], P(('pb', 'pa')), may hold values from 0 to 30, all different within a row; in each aligned block of 32 rows (0 to 31, 32 to 63, ...) at most 8 rows name the same one
- positive: int32 [4096], P(('pb', 'pa')), may hold values from 0 to 511
- context: bfloat16 [16384, 3584], P(('pb', 'pa')), may hold values from -6 to 6
- residual: bfloat16 [16384, 3584], P(('pb', 'pa')), may hold values from -6 to 6
- output_weight: bfloat16 [3584, 3584], P(('pb', 'pa')), may hold values from -0.09375 to 0.09375
- adapter_down_weight: bfloat16 [3584, 16], replicated, may hold values from -0.09375 to 0.09375
- adapter_up_weight: bfloat16 [16, 3584], replicated, may hold values from -1.5 to 1.5
- final_norm_weight: bfloat16 [3584], replicated, may hold values from 0.099609375 to 1.8984375
Outputs:
- query_gradient: float32 [4096, 3584], P(('pb', 'pa'))
- grad_passages: float32 [16384, 3584], P(('pb', 'pa'))
- grad_lora_down: float32 [3584, 16], P(('pb', 'pa'))
- grad_lora_up: float32 [16, 3584], P(None, ('pb', 'pa'))
The draws below stay inside these ranges and needn't reach their ends.
Inputs may be any that keep to these rules, and one draw needn't show every extreme that they name: `hard_block_offsets`: each row lists 4 different offsets. Query block k is paired with passage block (k // 32 + 1 + offset) modulo the number of devices. In each aligned block of 32 rows no offset appears more than 8 times, and some offset appears exactly 8 times.
All inputs are finite; a program needn't handle non-finite values.
Results may differ from the reference program's by a relative error of at most 0.0045.
Values may be sent and summed in bfloat16 or wider, within the bound.
No kernel may reach another device: no remote copies, remote signals or barrier semaphores. Data moves between devices by JAX's collectives and lax.ppermute only.
A program may use at most 192 MiB of HBM per device.

```python
import math
import jax
import jax.numpy as jnp
import numpy as np
from jax import lax

MODEL_WIDTH = 3584
QBLOCKS = 32
BLOCK_ROWS = 4
HARD = 4
PASS_DEV = 512
ADAPTER_RANK = 16
RERUN_QUERIES = 16
TQ = 32
CAP = 8
NQ = 4096
NQB = 1024
NP = 16384
TOKENS = 16384
N_PB = 4
N_PA = 8


def embedding_pair(key):
    seeded = jax.random.fold_in(key, 5501)
    key_query, key_passage = jax.random.split(seeded, 2)
    queries = jax.random.normal(key_query, (NQ, MODEL_WIDTH), jnp.float32)
    passages = jax.random.normal(key_passage, (NP, MODEL_WIDTH), jnp.float32)
    return (jnp.clip(queries, -16.0, 16.0), jnp.clip(passages, -16.0, 16.0))


def draw_queries(key, part):
    return embedding_pair(key)[0].astype(jnp.bfloat16)


def draw_passages(key, part):
    return embedding_pair(key)[1].astype(jnp.bfloat16)


def plant(values, stream_key, smallest, largest):
    extent = values.shape
    spot = [jax.random.randint(jax.random.fold_in(stream_key, axis), (), 0, extent[axis]) for axis in range(len(extent))]
    values = values.at[tuple(spot)].set(smallest)
    longest = extent.index(max(extent))
    spot[longest] = (spot[longest] + 1) % extent[longest]
    return values.at[tuple(spot)].set(largest)


def strengthened(values, rng, source, target, parts, factor):
    def block_of(axis_at):
        return (jnp.arange(values.shape[axis_at]) // (values.shape[axis_at] // parts)).reshape((-1,) + (1,) * (values.ndim - 1 - axis_at))

    near = jax.random.permutation(rng, parts)[block_of(target)]
    far = (block_of(target) + parts // 2) % parts
    return jnp.where((block_of(source) == near) | (block_of(source) == far), factor * values, values)


def level_of(rng, shape, cuts, smallest, high):
    factor_of, own = 1.0, jax.random.fold_in(rng, 6)
    for dim, parts in cuts:
        steps = jnp.exp(jax.random.uniform(jax.random.fold_in(own, dim), (parts,), jnp.float32, smallest / len(cuts), high / len(cuts)))
        factor_of = factor_of * jnp.repeat(steps, shape[dim] // parts).reshape([-1 if axis == dim else 1 for axis in range(len(shape))])
    return factor_of


def deal_out(own_key, own, number, rows, count, top, limit, lean):
    sequence = jax.random.permutation(own_key, count)
    crowded, usual = shares(count, rows * top, limit, lean, True), shares(count, rows * top, limit, lean, False)
    places = jnp.arange(count)

    def named(tallies, turn):
        used = int((tallies > 0).sum())
        fixed = max(1, used // 4)
        moved = fixed + (places - fixed + turn * (used - fixed)) % max(1, count - fixed)
        return jnp.zeros((count,), jnp.int32).at[sequence[jnp.where(places < fixed, places, moved)]].set(jnp.asarray(tallies, jnp.int32))

    tallies = jnp.where(number % 4 == 0, named(crowded, number // 4), named(usual, number - number // 4 - 1))
    mixed = jax.random.permutation(jax.random.fold_in(own, 3), count)
    donor, sink = mixed[0:count // 2 * 2:2], mixed[1:count // 2 * 2:2]
    room = jnp.minimum(tallies[donor] - 1, limit - tallies[sink]) // 2
    room = jnp.where((donor == sequence[0]) | (sink == sequence[0]) | (tallies[sink] == 0), 0, jnp.maximum(room, 0))
    moved = jax.random.randint(jax.random.fold_in(own, 4), (count // 2,), 0, 1 << 20) % (room + 1)
    tallies = tallies.at[donor].add(-moved).at[sink].add(moved)
    members = jnp.searchsorted(jnp.cumsum(tallies), jnp.arange(rows * top), side="right").astype(jnp.int32)
    listing = members.reshape(top, rows).T
    listing = listing[jax.random.permutation(jax.random.fold_in(own, 1), rows)]
    turn = jax.random.randint(jax.random.fold_in(own, 2), (rows, 1), 0, top)
    return jnp.take_along_axis(listing, (jnp.arange(top)[None, :] + turn) % top, axis=1)


def shares(amount, total, reach, slope, full):
    portions = [(1 << 20) // math.isqrt(rank ** slope) + 1 for rank in range(1, amount + 1)]
    largest = reach if full else min(reach, max(-(-total // amount), total * portions[0] // sum(portions)))
    least = 1 if total - largest >= amount - 1 else 0
    holding, surplus = [largest] + [least] * (amount - 1), total - largest - least * (amount - 1)
    while surplus > 0:
        free = [i for i in range(1, amount) if holding[i] < largest] or [i for i in range(1, amount) if holding[i] < reach]
        pool, budget = sum([portions[i] for i in free]), surplus
        for i in free:
            addition = min(reach - holding[i], max(1, budget * portions[i] // pool), surplus)
            holding[i] = holding[i] + addition
            surplus = surplus - addition
    return np.array(holding)


def normal_values(own_key, shape, scale, limit, cuts=(), held_as=jnp.bfloat16):
    values = scale * jax.random.normal(own_key, shape, jnp.float32)
    if cuts:
        values = values * level_of(own_key, shape, cuts, -0.22, 0.18)
    return jnp.clip(values, -limit, limit).astype(held_as)


def noise_with(stream_key, extent, width, reach, cuts, heavy, kind=jnp.bfloat16):
    values = width * jax.random.normal(stream_key, extent, jnp.float32)
    if cuts:
        values = values * level_of(stream_key, extent, cuts, -0.22, 0.18)
    return jnp.clip(strengthened(values, jax.random.fold_in(stream_key, 3), *heavy), -reach, reach).astype(kind)


def setup_inputs(seed: int = 0) -> dict:
    keys = jax.random.split(jax.random.key(seed), 11)
    queries = draw_queries(jax.random.fold_in(keys[10], 71), 0)
    passages = draw_passages(jax.random.fold_in(keys[10], 71), 0)
    hard_block_offsets_keys = jax.random.split(jax.random.fold_in(keys[2], 1), NQB // QBLOCKS)
    hard_block_offsets_turns = jax.random.permutation(jax.random.fold_in(keys[2], 3), NQB // QBLOCKS)
    hard_block_offsets = jax.vmap(lambda own, number: deal_out(jax.random.fold_in(keys[2], 2), own, number, QBLOCKS, N_PB * N_PA - 1, HARD, CAP, 2))(hard_block_offsets_keys, hard_block_offsets_turns).reshape((NQB, HARD))
    positive = plant(jax.random.randint(keys[3], (NQ,), 0, PASS_DEV), jax.random.fold_in(keys[3], 1), 0, PASS_DEV - 1).astype(jnp.int32)
    context = noise_with(keys[4], (TOKENS, MODEL_WIDTH), 1.0, 6.0, ((0, 32),), (0, 1, 32, 2.75))
    residual = normal_values(keys[5], (TOKENS, MODEL_WIDTH), 1.0, 6.0, ((0, 32),))
    output_weight = normal_values(keys[6], (MODEL_WIDTH, MODEL_WIDTH), MODEL_WIDTH ** -0.5, 0.09375, ((0, 32),))
    adapter_down_weight = normal_values(keys[7], (MODEL_WIDTH, ADAPTER_RANK), MODEL_WIDTH ** -0.5, 0.09375)
    adapter_up_weight = normal_values(keys[8], (ADAPTER_RANK, MODEL_WIDTH), ADAPTER_RANK ** -0.5, 1.5)
    final_norm_weight = jnp.clip(1.0 + 0.18 * jax.random.normal(keys[9], (MODEL_WIDTH,), jnp.float32), 0.099609375, 1.8984375).astype(jnp.bfloat16)
    return {"queries": queries, "passages": passages, "hard_block_offsets": hard_block_offsets, "positive": positive, "context": context, "residual": residual, "output_weight": output_weight, "adapter_down_weight": adapter_down_weight, "adapter_up_weight": adapter_up_weight, "final_norm_weight": final_norm_weight}


inverse_temp = 2.0
loss_scale = 32.0
adapter_scale = 2.0
epsilon = 1e-06
absent_mass = 1e+30

def slot_layout(offsets, source, device_count, capacity):
    flat_offsets = offsets.reshape(-1)
    target = (source + 1 + flat_offsets) % device_count
    pair_order = jnp.arange(flat_offsets.shape[0], dtype=jnp.int32)
    earlier = (target[:, None] == target[None, :]) & (pair_order[:, None] > pair_order[None, :])
    slot_rank = lax.optimization_barrier(jnp.sum(earlier.astype(jnp.int32), axis=1)).astype(jnp.int32)
    slot_index = (target * capacity + slot_rank).astype(jnp.int32)
    slot_block = jnp.full((device_count * capacity,), -1, jnp.int32).at[slot_index].set(pair_order // offsets.shape[1])
    return (slot_index, slot_block)

def partial_softmax(query_rows, passage_rows, score_scale):
    scores = jnp.dot(query_rows, passage_rows.T, preferred_element_type=jnp.float32) * score_scale
    row_peak = lax.optimization_barrier(jnp.max(scores, axis=1))
    weights = jnp.exp(scores - row_peak[:, None])
    row_mass = lax.optimization_barrier(jnp.sum(weights, axis=1))
    row_mean = jnp.dot(weights.astype(jnp.bfloat16), passage_rows, preferred_element_type=jnp.float32) / row_mass[:, None]
    return (scores, row_peak + jnp.log(row_mass), row_mean)

def merge_partials(near_mass, near_mean, far_mass, far_mean):
    block_count, hard_count, block_rows = far_mass.shape
    far_rows = jnp.transpose(far_mass, (0, 2, 1)).reshape(block_count * block_rows, hard_count)
    every_mass = jnp.concatenate([near_mass[:, None], far_rows], axis=1)
    mass_peak = lax.optimization_barrier(jnp.max(every_mass, axis=1))
    log_total = mass_peak + jnp.log(lax.optimization_barrier(jnp.sum(jnp.exp(every_mass - mass_peak[:, None]), axis=1)))
    near_share = jnp.exp(near_mass - log_total)
    far_share = jnp.exp(far_mass - log_total.reshape(block_count, 1, block_rows))
    far_part = lax.optimization_barrier(jnp.sum(far_mean * far_share[..., None], axis=1)).reshape(block_count * block_rows, -1)
    return (log_total, near_share[:, None] * near_mean + far_part)

def layer_parts(context, residual, frozen_output, adapter_down_weight, adapter_up_weight, final_norm_weight, output_gradient):
    token_count = context.shape[0]
    narrow_projection = jnp.dot(context, adapter_down_weight, preferred_element_type=jnp.float32).astype(jnp.bfloat16)
    hidden_state = residual.astype(jnp.float32) + frozen_output + adapter_scale * jnp.dot(narrow_projection, adapter_up_weight, preferred_element_type=jnp.float32)
    inverse_rms = lax.rsqrt(lax.optimization_barrier(jnp.mean(hidden_state * hidden_state, axis=1, keepdims=True)) + epsilon)
    spread_cot = jnp.broadcast_to(output_gradient[:, None, :] / TQ, (output_gradient.shape[0], TQ, output_gradient.shape[1])).reshape(token_count, -1)
    scaled = final_norm_weight.astype(jnp.float32)[None, :] * spread_cot
    grad_hidden = inverse_rms * scaled - hidden_state * inverse_rms ** 3 * lax.optimization_barrier(jnp.mean(hidden_state * scaled, axis=1, keepdims=True))
    gradient_lowered = grad_hidden.astype(jnp.bfloat16)
    product_dims = (((0,), (0,)), ((), ()))
    up_product = adapter_scale * lax.dot_general(narrow_projection, gradient_lowered, product_dims, preferred_element_type=jnp.float32) / RERUN_QUERIES
    gradient_narrow = (adapter_scale * jnp.dot(gradient_lowered, adapter_up_weight.T, preferred_element_type=jnp.float32)).astype(jnp.bfloat16)
    down_term = lax.dot_general(context, gradient_narrow, product_dims, preferred_element_type=jnp.float32) / RERUN_QUERIES
    return (down_term, up_product)

def reference(queries, passages, hard_block_offsets, positive, context, residual, output_weight, adapter_down_weight, adapter_up_weight, final_norm_weight):
    device_count = N_PB * N_PA
    capacity = CAP
    query_count = QBLOCKS * BLOCK_ROWS
    score_scale = inverse_temp / math.sqrt(MODEL_WIDTH)
    query_grid = queries.reshape(device_count, query_count, MODEL_WIDTH)
    passage_grid = passages.reshape(device_count, PASS_DEV, MODEL_WIDTH)
    offset_grid = hard_block_offsets.reshape(device_count, QBLOCKS, HARD)
    sources = jnp.arange(device_count, dtype=jnp.int32)
    slot_grid, holder_grid = jax.vmap(lambda offsets, source: slot_layout(offsets, source, device_count, capacity))(offset_grid, sources)
    query_blocks = query_grid.reshape(device_count, QBLOCKS, BLOCK_ROWS, MODEL_WIDTH)

    def gather_slots(owner_index):
        slot_blocks = lax.dynamic_slice_in_dim(holder_grid, owner_index * capacity, capacity, 1)
        picked = query_blocks[sources[:, None], jnp.maximum(slot_blocks, 0)]
        picked = jnp.where((slot_blocks >= 0)[:, :, None, None], picked, jnp.zeros_like(picked))
        return (picked.reshape(-1, MODEL_WIDTH), slot_blocks)

    def owner_forward(owner_index):
        picked, slot_blocks = gather_slots(owner_index)
        scores, row_mass, row_mean = partial_softmax(picked, passage_grid[owner_index], score_scale)
        return (row_mass, row_mean.astype(jnp.bfloat16))
    far_masses, far_means = lax.map(owner_forward, sources)
    owner_grid = slot_grid // capacity
    place_grid = (sources[:, None] * capacity + slot_grid % capacity) * BLOCK_ROWS
    row_offsets = jnp.arange(BLOCK_ROWS, dtype=jnp.int32)
    far_mass_all = far_masses[owner_grid[:, :, None], place_grid[:, :, None] + row_offsets[None, None, :]]
    far_mean_all = far_means[owner_grid[:, :, None], place_grid[:, :, None] + row_offsets[None, None, :]]

    def query_side(pieces):
        own_queries, own_passages, own_positive, far_mass, far_mean = pieces
        near_scores, near_mass, near_mean = partial_softmax(own_queries, own_passages, score_scale)
        far_mass = far_mass.reshape(QBLOCKS, HARD, BLOCK_ROWS)
        far_mean = far_mean.reshape(QBLOCKS, HARD, BLOCK_ROWS, MODEL_WIDTH)
        log_total, mixed = merge_partials(near_mass, near_mean, far_mass, far_mean)
        positive_hot = own_positive[:, None] == jnp.arange(PASS_DEV, dtype=jnp.int32)[None, :]
        positive_rows = jnp.dot(positive_hot.astype(jnp.bfloat16), own_passages, preferred_element_type=jnp.float32)
        return (loss_scale * score_scale * (mixed - positive_rows), log_total)
    grads_q, log_totals = lax.map(query_side, (query_grid, passage_grid, positive.reshape(device_count, query_count), far_mass_all, far_mean_all))
    log_blocks = log_totals.reshape(device_count, QBLOCKS, BLOCK_ROWS)

    def owner_backward(pieces):
        owner_index, own_queries, own_passages, own_positive, own_log = pieces
        picked, slot_blocks = gather_slots(owner_index)
        far_log = log_blocks[sources[:, None], jnp.maximum(slot_blocks, 0)]
        far_log = jnp.where((slot_blocks >= 0)[:, :, None], far_log, absent_mass).reshape(-1)
        far_scores = jnp.dot(picked, own_passages.T, preferred_element_type=jnp.float32) * score_scale
        far_weight = jnp.exp(far_scores - far_log[:, None]).astype(jnp.bfloat16)
        near_scores = jnp.dot(own_queries, own_passages.T, preferred_element_type=jnp.float32) * score_scale
        positive_hot = own_positive[:, None] == jnp.arange(PASS_DEV, dtype=jnp.int32)[None, :]
        near_weight = (jnp.exp(near_scores - own_log[:, None]) - positive_hot.astype(jnp.float32)).astype(jnp.bfloat16)
        product_dims = (((0,), (0,)), ((), ()))
        far_grad = lax.dot_general(far_weight, picked, product_dims, preferred_element_type=jnp.float32)
        near_grad = lax.dot_general(near_weight, own_queries, product_dims, preferred_element_type=jnp.float32)
        return loss_scale * score_scale * (far_grad + near_grad)
    grads_p = lax.map(owner_backward, (sources, query_grid, passage_grid, positive.reshape(device_count, query_count), log_totals))
    cotangents = grads_q[:, :RERUN_QUERIES]
    context_grid = context.reshape(device_count, RERUN_QUERIES * TQ, MODEL_WIDTH)
    residual_grid = residual.reshape(device_count, RERUN_QUERIES * TQ, MODEL_WIDTH)

    def device_layer(pieces):
        local_context, local_residual, output_gradient = pieces
        frozen_output = jnp.dot(local_context, output_weight, preferred_element_type=jnp.float32)
        return layer_parts(local_context, local_residual, frozen_output, adapter_down_weight, adapter_up_weight, final_norm_weight, output_gradient)
    down_terms, up_terms = lax.map(device_layer, (context_grid, residual_grid, cotangents))
    return (grads_q.reshape(-1, MODEL_WIDTH), grads_p.reshape(-1, MODEL_WIDTH), lax.optimization_barrier(jnp.sum(down_terms, axis=0)), lax.optimization_barrier(jnp.sum(up_terms, axis=0)))
```

```python
import math

import jax
import jax.numpy as jnp
from jax import lax
from jax.sharding import PartitionSpec as P


MODEL_WIDTH = 3584
RERUN_QUERIES = 16
TQ = 32


inverse_temp = 2.0
loss_scale = 32.0
adapter_scale = 2.0
epsilon = 1e-06
absent_mass = 1e30


def slot_positions(offsets, source, device_count, capacity, block_rows):
    block_count, hard_count = offsets.shape
    flat_offsets = offsets.reshape(-1)
    target = (source + 1 + flat_offsets) % device_count
    pair_order = jnp.arange(flat_offsets.shape[0], dtype=jnp.int32)
    earlier = (target[:, None] == target[None, :]) & (pair_order[:, None] > pair_order[None, :])
    slot_rank = jnp.sum(earlier.astype(jnp.int32), axis=1)
    slot_index = (target * capacity + slot_rank).reshape(block_count, 1, hard_count)
    row = jnp.arange(block_rows, dtype=jnp.int32)[None, :, None]
    return (slot_index * block_rows + row).reshape(block_count * block_rows, hard_count)


def partial_softmax(query_rows, passage_rows, score_scale):
    scores = jnp.dot(query_rows, passage_rows.T, preferred_element_type=jnp.float32) * score_scale
    row_peak = jnp.max(scores, axis=1)
    weights = jnp.exp(scores - row_peak[:, None])
    row_mass = jnp.sum(weights, axis=1)
    row_mean = (
        jnp.dot(weights.astype(jnp.bfloat16), passage_rows, preferred_element_type=jnp.float32)
        / row_mass[:, None]
    )
    return (scores, row_peak + jnp.log(row_mass), row_mean)


def exchange(values):
    return lax.all_to_all(values, ("pb", "pa"), split_axis=0, concat_axis=0, tiled=True)


def layer_hidden(context, residual, whole_weight, adapter_down_weight, adapter_up_weight):
    narrow_projection = jnp.dot(
        context, adapter_down_weight, preferred_element_type=jnp.float32
    ).astype(jnp.bfloat16)
    frozen_output = jnp.dot(context, whole_weight, preferred_element_type=jnp.float32)
    hidden_state = (
        residual.astype(jnp.float32)
        + frozen_output
        + adapter_scale
        * jnp.dot(narrow_projection, adapter_up_weight, preferred_element_type=jnp.float32)
    )
    return (narrow_projection, hidden_state)


def layer_parts(
    context,
    narrow_projection,
    hidden_state,
    adapter_up_weight,
    final_norm_weight,
    output_gradient,
):
    token_count = context.shape[0]
    inverse_rms = lax.rsqrt(jnp.mean(hidden_state * hidden_state, axis=1, keepdims=True) + epsilon)
    spread_cot = jnp.broadcast_to(
        output_gradient[:, None, :] / TQ, (output_gradient.shape[0], TQ, output_gradient.shape[1])
    ).reshape(token_count, -1)
    scaled = final_norm_weight.astype(jnp.float32)[None, :] * spread_cot
    grad_hidden = inverse_rms * scaled - hidden_state * inverse_rms**3 * jnp.mean(
        hidden_state * scaled, axis=1, keepdims=True
    )
    gradient_lowered = grad_hidden.astype(jnp.bfloat16)
    product_dims = (((0,), (0,)), ((), ()))
    up_product = lax.dot_general(
        narrow_projection, gradient_lowered, product_dims, preferred_element_type=jnp.float32
    ) * (adapter_scale / RERUN_QUERIES)
    gradient_narrow = (
        adapter_scale
        * jnp.dot(gradient_lowered, adapter_up_weight.T, preferred_element_type=jnp.float32)
    ).astype(jnp.bfloat16)
    down_product = lax.dot_general(
        gradient_narrow, context, product_dims, preferred_element_type=jnp.float32
    ) * (1.0 / RERUN_QUERIES)
    return (down_product, up_product)


def local_step(
    queries,
    passages,
    hard_block_offsets,
    positive,
    context,
    residual,
    output_weight,
    adapter_down_weight,
    adapter_up_weight,
    final_norm_weight,
):
    device_count = lax.axis_size(("pb", "pa"))
    block_count, hard_count = hard_block_offsets.shape
    query_count = queries.shape[0]
    block_rows = query_count // block_count
    capacity = 2 * block_count * hard_count // device_count
    slot_width = capacity * block_rows
    slot_rows = device_count * slot_width
    passage_count = passages.shape[0]
    score_scale = inverse_temp / math.sqrt(MODEL_WIDTH)
    own_index = lax.axis_index(("pb", "pa"))
    place = slot_positions(hard_block_offsets, own_index, device_count, capacity, block_rows)
    slot_row = jnp.arange(slot_rows, dtype=jnp.int32)
    sent = slot_row[:, None, None] == place[None]
    sent_row = jnp.any(sent, axis=2)
    outgoing = jnp.dot(
        sent_row.astype(jnp.bfloat16), queries, preferred_element_type=jnp.float32
    ).astype(jnp.bfloat16)
    arrived = exchange(outgoing.reshape(device_count, slot_width, MODEL_WIDTH))
    arrived = arrived.reshape(-1, MODEL_WIDTH)
    whole_weight = lax.all_gather(output_weight, ("pb", "pa"), axis=0, tiled=True)
    near_scores, near_mass, near_mean = partial_softmax(queries, passages, score_scale)
    far_scores, far_mass, far_mean = partial_softmax(arrived, passages, score_scale)
    returned_mass = exchange(far_mass.reshape(device_count, slot_width)).reshape(-1)
    returned_mean = exchange(
        far_mean.astype(jnp.bfloat16).reshape(device_count, slot_width, MODEL_WIDTH)
    )
    returned_mean = returned_mean.reshape(-1, MODEL_WIDTH)
    narrow_projection, hidden_state = layer_hidden(
        context, residual, whole_weight, adapter_down_weight, adapter_up_weight
    )
    held = place[:, :, None] == slot_row[None, None, :]
    own_far_mass = jnp.sum(jnp.where(held, returned_mass[None, None, :], 0.0), axis=2)
    every_mass = jnp.concatenate([near_mass[:, None], own_far_mass], axis=1)
    mass_peak = jnp.max(every_mass, axis=1)
    log_total = mass_peak + jnp.log(jnp.sum(jnp.exp(every_mass - mass_peak[:, None]), axis=1))
    near_share = jnp.exp(near_mass - log_total)
    far_share = jnp.exp(own_far_mass - log_total[:, None])
    log_outgoing = jnp.where(
        jnp.any(sent_row, axis=1),
        jnp.sum(jnp.where(sent_row, log_total[None, :], 0.0), axis=1),
        absent_mass,
    )
    log_arrived = exchange(log_outgoing.reshape(device_count, slot_width)).reshape(-1)
    share_rows = jnp.sum(jnp.where(held, far_share[:, :, None], 0.0), axis=1)
    share_high = lax.reduce_precision(share_rows, 8, 7)
    share_parts = jnp.concatenate([share_high, share_rows - share_high], axis=0)
    mixed_parts = jnp.dot(
        share_parts.astype(jnp.bfloat16), returned_mean, preferred_element_type=jnp.float32
    )
    far_part = mixed_parts[:query_count] + mixed_parts[query_count:]
    positive_hot = positive[:, None] == jnp.arange(passage_count, dtype=jnp.int32)[None, :]
    positive_rows = jnp.dot(
        positive_hot.astype(jnp.bfloat16), passages, preferred_element_type=jnp.float32
    )
    own_part = near_share[:, None] * near_mean - positive_rows
    query_gradient = loss_scale * score_scale * (far_part + own_part)
    far_weight = jnp.exp(far_scores - log_arrived[:, None]).astype(jnp.bfloat16)
    near_weight = (
        jnp.exp(near_scores - log_total[:, None]) - positive_hot.astype(jnp.float32)
    ).astype(jnp.bfloat16)
    product_dims = (((0,), (0,)), ((), ()))
    far_grad = lax.dot_general(
        far_weight, arrived, product_dims, preferred_element_type=jnp.float32
    )
    near_grad = lax.dot_general(
        near_weight, queries, product_dims, preferred_element_type=jnp.float32
    )
    grad_passages = loss_scale * score_scale * (far_grad + near_grad)
    down_product, up_product = layer_parts(
        context,
        narrow_projection,
        hidden_state,
        adapter_up_weight,
        final_norm_weight,
        query_gradient[:RERUN_QUERIES],
    )
    rank = up_product.shape[0]
    adapter_terms = jnp.concatenate([down_product, up_product], axis=0)
    adapter_terms = adapter_terms.reshape(2 * rank, device_count, -1).transpose(1, 0, 2)
    adapter_sums = jnp.sum(exchange(adapter_terms), axis=0)
    return (query_gradient, grad_passages, adapter_sums[:rank].T, adapter_sums[rank:])


def solution(mesh):
    placed = (
        P(("pb", "pa"), None),
        P(("pb", "pa"), None),
        P(("pb", "pa"), None),
        P(("pb", "pa")),
        P(("pb", "pa"), None),
        P(("pb", "pa"), None),
        P(("pb", "pa"), None),
        P(),
        P(),
        P(),
    )
    return jax.shard_map(
        local_step,
        mesh=mesh,
        in_specs=placed,
        out_specs=(
            P(("pb", "pa"), None),
            P(("pb", "pa"), None),
            P(("pb", "pa"), None),
            P(None, ("pb", "pa")),
        ),
        check_vma=False,
    )
```

```python
import math

import jax
import jax.numpy as jnp
from jax import lax
from jax.sharding import PartitionSpec as P


MODEL_WIDTH = 3584
RERUN_QUERIES = 16
TQ = 32


inverse_temp = 2.0
loss_scale = 32.0
adapter_scale = 2.0
epsilon = 1e-06
absent_mass = 1e30


def slot_positions(offsets, source, device_count, capacity, block_rows):
    block_count, hard_count = offsets.shape
    flat_offsets = offsets.reshape(-1)
    target = (source + 1 + flat_offsets) % device_count
    pair_order = jnp.arange(flat_offsets.shape[0], dtype=jnp.int32)
    earlier = (target[:, None] == target[None, :]) & (pair_order[:, None] > pair_order[None, :])
    slot_rank = jnp.sum(earlier.astype(jnp.int32), axis=1)
    slot_index = (target * capacity + slot_rank).reshape(block_count, 1, hard_count)
    row = jnp.arange(block_rows, dtype=jnp.int32)[None, :, None]
    return (slot_index * block_rows + row).reshape(block_count * block_rows, hard_count)


def partial_softmax(query_rows, passage_rows, score_scale):
    scores = jnp.dot(query_rows, passage_rows.T, preferred_element_type=jnp.float32) * score_scale
    row_peak = jnp.max(scores, axis=1)
    weights = jnp.exp(scores - row_peak[:, None])
    row_mass = jnp.sum(weights, axis=1)
    row_mean = (
        jnp.dot(weights.astype(jnp.bfloat16), passage_rows, preferred_element_type=jnp.float32)
        / row_mass[:, None]
    )
    return (scores, row_peak + jnp.log(row_mass), row_mean)


def exchange(values, axes):
    return lax.all_to_all(values, axes, split_axis=0, concat_axis=0, tiled=True)


def arrival_table(count):
    table = []
    for place in range(count):
        others = sorted(range(count), key=lambda other: (abs(other - place), other))
        table.append(others)
    return table


def relay_planes(rows, plane, count):
    table = arrival_table(count)
    below, above = [rows], [rows]
    for step in range(1, count):
        up = [(i, i + 1) for i in range(step - 1, count - 1)]
        down = [(i + 1, i) for i in range(count - step)]
        below.append(lax.ppermute(below[-1], "pb", up))
        above.append(lax.ppermute(above[-1], "pb", down))
    chunks = []
    for order in range(count):
        source = jnp.array([row[order] for row in table], jnp.int32)[plane]
        picked = None
        for place in range(count):
            shift = place - table[place][order]
            candidate = below[shift] if shift >= 0 else above[-shift]
            picked = candidate if picked is None else jnp.where(plane == place, candidate, picked)
        chunks.append((source, picked))
    return chunks


def chosen(parts, index):
    result = parts[0]
    for number in range(1, len(parts)):
        result = jnp.where(index == number, parts[number], result)
    return result


def layer_hidden(context, residual, whole_weight, adapter_down_weight, adapter_up_weight):
    narrow_projection = jnp.dot(
        context, adapter_down_weight, preferred_element_type=jnp.float32
    ).astype(jnp.bfloat16)
    frozen_output = jnp.dot(context, whole_weight, preferred_element_type=jnp.float32)
    hidden_state = (
        residual.astype(jnp.float32)
        + frozen_output
        + adapter_scale
        * jnp.dot(narrow_projection, adapter_up_weight, preferred_element_type=jnp.float32)
    )
    return (narrow_projection, hidden_state)


def layer_parts(
    context,
    narrow_projection,
    hidden_state,
    adapter_up_weight,
    final_norm_weight,
    output_gradient,
):
    token_count = context.shape[0]
    inverse_rms = lax.rsqrt(jnp.mean(hidden_state * hidden_state, axis=1, keepdims=True) + epsilon)
    spread_cot = jnp.broadcast_to(
        output_gradient[:, None, :] / TQ, (output_gradient.shape[0], TQ, output_gradient.shape[1])
    ).reshape(token_count, -1)
    scaled = final_norm_weight.astype(jnp.float32)[None, :] * spread_cot
    grad_hidden = inverse_rms * scaled - hidden_state * inverse_rms**3 * jnp.mean(
        hidden_state * scaled, axis=1, keepdims=True
    )
    gradient_lowered = grad_hidden.astype(jnp.bfloat16)
    product_dims = (((0,), (0,)), ((), ()))
    up_product = lax.dot_general(
        narrow_projection, gradient_lowered, product_dims, preferred_element_type=jnp.float32
    ) * (adapter_scale / RERUN_QUERIES)
    gradient_narrow = (
        adapter_scale
        * jnp.dot(gradient_lowered, adapter_up_weight.T, preferred_element_type=jnp.float32)
    ).astype(jnp.bfloat16)
    down_product = lax.dot_general(
        gradient_narrow, context, product_dims, preferred_element_type=jnp.float32
    ) * (1.0 / RERUN_QUERIES)
    return (down_product, up_product)


def local_step(
    queries,
    passages,
    hard_block_offsets,
    positive,
    context,
    residual,
    output_weight,
    adapter_down_weight,
    adapter_up_weight,
    final_norm_weight,
):
    plane_count, column_count = lax.axis_size("pb"), lax.axis_size("pa")
    plane, column = lax.axis_index("pb"), lax.axis_index("pa")
    device_count = plane_count * column_count
    block_count, hard_count = hard_block_offsets.shape
    query_count = queries.shape[0]
    block_rows = query_count // block_count
    capacity = 2 * block_count * hard_count // device_count
    slot_width = capacity * block_rows
    slot_rows = device_count * slot_width
    plane_rows = column_count * slot_width
    passage_count = passages.shape[0]
    score_scale = inverse_temp / math.sqrt(MODEL_WIDTH)
    chunks = relay_planes(queries, plane, plane_count)
    whole_weight = lax.all_gather(output_weight, ("pb", "pa"), axis=0, tiled=True)
    plane_places = []
    for shift in range(plane_count):
        offsets = hard_block_offsets
        if shift:
            offsets = lax.ppermute(
                offsets, "pb", [(i, (i + shift) % plane_count) for i in range(plane_count)]
            )
        source = (plane - shift) % plane_count * column_count + column
        plane_places.append(
            slot_positions(offsets, source, device_count, capacity, block_rows)
        )
    own_place = plane_places[0]
    plane_row = jnp.arange(plane_rows, dtype=jnp.int32)

    def plane_hot(source, place=None):
        if place is None:
            place = chosen(plane_places, (plane - source) % plane_count)
        place = place - plane * plane_rows
        return jnp.any(plane_row[:, None, None] == place[None], axis=2)

    arrived, far_scores, far_mass = [], [], []
    for order, (source, rows) in enumerate(chunks):
        packed = jnp.dot(
            plane_hot(source, None if order else own_place).astype(jnp.bfloat16), rows, preferred_element_type=jnp.float32
        ).astype(jnp.bfloat16)
        landed = exchange(packed.reshape(column_count, slot_width, MODEL_WIDTH), "pa")
        landed = landed.reshape(plane_rows, MODEL_WIDTH)
        scores = (
            jnp.dot(landed, passages.T, preferred_element_type=jnp.float32) * score_scale
        )
        peak = jnp.max(scores, axis=1)
        mass = peak + jnp.log(jnp.sum(jnp.exp(scores - peak[:, None]), axis=1))
        arrived.append(landed)
        far_scores.append(scores)
        far_mass.append(mass)
    near_scores, near_mass, near_mean = partial_softmax(queries, passages, score_scale)
    orders = jnp.array(
        [[row.index(p) for p in range(plane_count)] for row in arrival_table(plane_count)],
        jnp.int32,
    )[plane]
    ordered_mass = jnp.stack([chosen(far_mass, orders[p]) for p in range(plane_count)])
    returned_mass = exchange(
        ordered_mass.reshape(device_count, slot_width), ("pb", "pa")
    ).reshape(-1)
    slot_row = jnp.arange(slot_rows, dtype=jnp.int32)
    held = own_place[:, :, None] == slot_row[None, None, :]
    own_far_mass = jnp.sum(jnp.where(held, returned_mass[None, None, :], 0.0), axis=2)
    every_mass = jnp.concatenate([near_mass[:, None], own_far_mass], axis=1)
    mass_peak = jnp.max(every_mass, axis=1)
    log_total = mass_peak + jnp.log(jnp.sum(jnp.exp(every_mass - mass_peak[:, None]), axis=1))
    near_share = jnp.exp(near_mass - log_total)
    sent_row = jnp.any(slot_row[:, None, None] == own_place[None], axis=2)
    log_outgoing = jnp.where(
        jnp.any(sent_row, axis=1),
        jnp.sum(jnp.where(sent_row, log_total[None, :], 0.0), axis=1),
        absent_mass,
    )
    log_arrived = exchange(
        log_outgoing.reshape(device_count, slot_width), ("pb", "pa")
    ).reshape(plane_count, plane_rows)
    far_weight = []
    for order, (source, _) in enumerate(chunks):
        log_rows = chosen([log_arrived[p] for p in range(plane_count)], source)
        far_weight.append(
            jnp.exp(far_scores[order] - log_rows[:, None]).astype(jnp.bfloat16)
        )
    shifts = sorted(range(plane_count), key=lambda k: -min(k, plane_count - k))
    far_part = None
    for shift in shifts:
        goal = (plane + shift) % plane_count
        weight_rows = chosen(far_weight, chosen([orders[p] for p in range(plane_count)], goal))
        share = jnp.dot(weight_rows, passages, preferred_element_type=jnp.float32)
        share = share.astype(jnp.bfloat16).reshape(column_count, slot_width, MODEL_WIDTH)
        share = exchange(share, "pa")
        merged = lax.dot_general(
            plane_hot(goal, None if shift else own_place).astype(jnp.bfloat16),
            share.reshape(plane_rows, MODEL_WIDTH),
            (((0,), (0,)), ((), ())),
            preferred_element_type=jnp.float32,
        )
        if shift:
            merged = lax.ppermute(
                merged.astype(jnp.bfloat16),
                "pb",
                [(i, (i + shift) % plane_count) for i in range(plane_count)],
            )
        far_part = merged.astype(jnp.float32) if far_part is None else far_part + merged.astype(jnp.float32)
    narrow_projection, hidden_state = layer_hidden(
        context, residual, whole_weight, adapter_down_weight, adapter_up_weight
    )
    positive_hot = positive[:, None] == jnp.arange(passage_count, dtype=jnp.int32)[None, :]
    positive_rows = jnp.dot(
        positive_hot.astype(jnp.bfloat16), passages, preferred_element_type=jnp.float32
    )
    own_part = near_share[:, None] * near_mean - positive_rows
    query_gradient = loss_scale * score_scale * (far_part + own_part)
    near_weight = (
        jnp.exp(near_scores - log_total[:, None]) - positive_hot.astype(jnp.float32)
    ).astype(jnp.bfloat16)
    product_dims = (((0,), (0,)), ((), ()))
    every_row = jnp.concatenate([queries] + arrived, axis=0)
    every_weight = jnp.concatenate([near_weight] + far_weight, axis=0)
    grad_passages = (loss_scale * score_scale) * lax.dot_general(
        every_weight, every_row, product_dims, preferred_element_type=jnp.float32
    )
    down_product, up_product = layer_parts(
        context,
        narrow_projection,
        hidden_state,
        adapter_up_weight,
        final_norm_weight,
        query_gradient[:RERUN_QUERIES],
    )
    rank = up_product.shape[0]
    adapter_terms = jnp.concatenate([down_product, up_product], axis=0)
    adapter_terms = adapter_terms.reshape(2 * rank, device_count, -1).transpose(1, 0, 2)
    adapter_sums = jnp.sum(
        exchange(adapter_terms.astype(jnp.bfloat16), ("pb", "pa")).astype(jnp.float32), axis=0
    )
    return (query_gradient, grad_passages, adapter_sums[:rank].T, adapter_sums[rank:])


def solution(mesh):
    placed = (
        P(("pb", "pa"), None),
        P(("pb", "pa"), None),
        P(("pb", "pa"), None),
        P(("pb", "pa")),
        P(("pb", "pa"), None),
        P(("pb", "pa"), None),
        P(("pb", "pa"), None),
        P(),
        P(),
        P(),
    )
    return jax.shard_map(
        local_step,
        mesh=mesh,
        in_specs=placed,
        out_specs=(
            P(("pb", "pa"), None),
            P(("pb", "pa"), None),
            P(("pb", "pa"), None),
            P(None, ("pb", "pa")),
        ),
        check_vma=False,
    )
```

```python
import math

import jax
import jax.numpy as jnp
from jax import lax
from jax.sharding import PartitionSpec as P


MODEL_WIDTH = 3584
RERUN_QUERIES = 16
TQ = 32


inverse_temp = 2.0
loss_scale = 32.0
adapter_scale = 2.0
epsilon = 1e-06
absent_mass = 1e30


def slot_positions(offsets, source, device_count, capacity, block_rows):
    block_count, hard_count = offsets.shape
    flat_offsets = offsets.reshape(-1)
    target = (source + 1 + flat_offsets) % device_count
    pair_order = jnp.arange(flat_offsets.shape[0], dtype=jnp.int32)
    earlier = (target[:, None] == target[None, :]) & (pair_order[:, None] > pair_order[None, :])
    slot_rank = jnp.sum(earlier.astype(jnp.int32), axis=1)
    slot_index = (target * capacity + slot_rank).reshape(block_count, 1, hard_count)
    row = jnp.arange(block_rows, dtype=jnp.int32)[None, :, None]
    return (slot_index * block_rows + row).reshape(block_count * block_rows, hard_count)


def partial_softmax(query_rows, passage_rows, score_scale):
    scores = jnp.dot(query_rows, passage_rows.T, preferred_element_type=jnp.float32) * score_scale
    row_peak = jnp.max(scores, axis=1)
    weights = jnp.exp(scores - row_peak[:, None])
    row_mass = jnp.sum(weights, axis=1)
    row_mean = (
        jnp.dot(weights.astype(jnp.bfloat16), passage_rows, preferred_element_type=jnp.float32)
        / row_mass[:, None]
    )
    return (scores, row_peak + jnp.log(row_mass), row_mean)


def exchange(values, axes):
    return lax.all_to_all(values, axes, split_axis=0, concat_axis=0, tiled=True)


def arrival_table(count):
    table = []
    for place in range(count):
        others = sorted(range(count), key=lambda other: (abs(other - place), other))
        table.append(others)
    return table


def relay_planes(rows, plane, count):
    table = arrival_table(count)
    below, above = [rows], [rows]
    for step in range(1, count):
        up = [(i, i + 1) for i in range(step - 1, count - 1)]
        down = [(i + 1, i) for i in range(count - step)]
        below.append(lax.ppermute(below[-1], "pb", up))
        above.append(lax.ppermute(above[-1], "pb", down))
    chunks = []
    for order in range(count):
        source = chosen([jnp.int32(row[order]) for row in table], plane)
        picked = None
        for place in range(count):
            shift = place - table[place][order]
            candidate = below[shift] if shift >= 0 else above[-shift]
            picked = candidate if picked is None else jnp.where(plane == place, candidate, picked)
        chunks.append((source, picked))
    return chunks


def chosen(parts, index):
    result = parts[0]
    for number in range(1, len(parts)):
        result = jnp.where(index == number, parts[number], result)
    return result


def layer_hidden(context, residual, whole_weight, adapter_down_weight, adapter_up_weight):
    narrow_projection = jnp.dot(
        context, adapter_down_weight, preferred_element_type=jnp.float32
    ).astype(jnp.bfloat16)
    frozen_output = jnp.dot(context, whole_weight, preferred_element_type=jnp.float32)
    hidden_state = (
        residual.astype(jnp.float32)
        + frozen_output
        + adapter_scale
        * jnp.dot(narrow_projection, adapter_up_weight, preferred_element_type=jnp.float32)
    )
    return (narrow_projection, hidden_state)


def layer_parts(
    context,
    narrow_projection,
    hidden_state,
    adapter_up_weight,
    final_norm_weight,
    output_gradient,
):
    token_count = context.shape[0]
    inverse_rms = lax.rsqrt(jnp.mean(hidden_state * hidden_state, axis=1, keepdims=True) + epsilon)
    spread_cot = jnp.broadcast_to(
        output_gradient[:, None, :] / TQ, (output_gradient.shape[0], TQ, output_gradient.shape[1])
    ).reshape(token_count, -1)
    scaled = final_norm_weight.astype(jnp.float32)[None, :] * spread_cot
    grad_hidden = inverse_rms * scaled - hidden_state * inverse_rms**3 * jnp.mean(
        hidden_state * scaled, axis=1, keepdims=True
    )
    gradient_lowered = grad_hidden.astype(jnp.bfloat16)
    product_dims = (((0,), (0,)), ((), ()))
    up_product = lax.dot_general(
        narrow_projection, gradient_lowered, product_dims, preferred_element_type=jnp.float32
    ) * (adapter_scale / RERUN_QUERIES)
    gradient_narrow = (
        adapter_scale
        * jnp.dot(gradient_lowered, adapter_up_weight.T, preferred_element_type=jnp.float32)
    ).astype(jnp.bfloat16)
    down_product = lax.dot_general(
        gradient_narrow, context, product_dims, preferred_element_type=jnp.float32
    ) * (1.0 / RERUN_QUERIES)
    return (down_product, up_product)


def local_step(
    queries,
    passages,
    hard_block_offsets,
    positive,
    context,
    residual,
    output_weight,
    adapter_down_weight,
    adapter_up_weight,
    final_norm_weight,
):
    plane_count, column_count = lax.axis_size("pb"), lax.axis_size("pa")
    plane, column = lax.axis_index("pb"), lax.axis_index("pa")
    device_count = plane_count * column_count
    block_count, hard_count = hard_block_offsets.shape
    query_count = queries.shape[0]
    block_rows = query_count // block_count
    capacity = 2 * block_count * hard_count // device_count
    slot_width = capacity * block_rows
    slot_rows = device_count * slot_width
    plane_rows = column_count * slot_width
    passage_count = passages.shape[0]
    score_scale = inverse_temp / math.sqrt(MODEL_WIDTH)
    chunks = relay_planes(queries, plane, plane_count)
    whole_weight = lax.all_gather(output_weight, ("pb", "pa"), axis=0, tiled=True)
    plane_places = []
    for shift in range(plane_count):
        offsets = hard_block_offsets
        if shift:
            offsets = lax.ppermute(
                offsets, "pb", [(i, (i + shift) % plane_count) for i in range(plane_count)]
            )
        source = (plane - shift) % plane_count * column_count + column
        plane_places.append(
            slot_positions(offsets, source, device_count, capacity, block_rows)
        )
    own_place = plane_places[0]
    plane_row = jnp.arange(plane_rows, dtype=jnp.int32)

    def plane_hot(source, place=None):
        if place is None:
            place = chosen(plane_places, (plane - source) % plane_count)
        place = place - plane * plane_rows
        return jnp.any(plane_row[:, None, None] == place[None], axis=2)

    arrived, far_scores, far_mass = [], [], []
    for order, (source, rows) in enumerate(chunks):
        packed = jnp.dot(
            plane_hot(source, None if order else own_place).astype(jnp.bfloat16), rows, preferred_element_type=jnp.float32
        ).astype(jnp.bfloat16)
        landed = exchange(packed.reshape(column_count, slot_width, MODEL_WIDTH), "pa")
        landed = landed.reshape(plane_rows, MODEL_WIDTH)
        scores = (
            jnp.dot(landed, passages.T, preferred_element_type=jnp.float32) * score_scale
        )
        peak = jnp.max(scores, axis=1)
        mass = peak + jnp.log(jnp.sum(jnp.exp(scores - peak[:, None]), axis=1))
        arrived.append(landed)
        far_scores.append(scores)
        far_mass.append(mass)
    near_scores, near_mass, near_mean = partial_softmax(queries, passages, score_scale)
    table = arrival_table(plane_count)
    orders = [
        chosen([jnp.int32(row.index(p)) for row in table], plane) for p in range(plane_count)
    ]
    ordered_mass = jnp.stack([chosen(far_mass, orders[p]) for p in range(plane_count)])
    returned_mass = exchange(
        ordered_mass.reshape(device_count, slot_width), ("pb", "pa")
    ).reshape(-1)
    slot_row = jnp.arange(slot_rows, dtype=jnp.int32)
    held = own_place[:, :, None] == slot_row[None, None, :]
    own_far_mass = jnp.sum(jnp.where(held, returned_mass[None, None, :], 0.0), axis=2)
    every_mass = jnp.concatenate([near_mass[:, None], own_far_mass], axis=1)
    mass_peak = jnp.max(every_mass, axis=1)
    log_total = mass_peak + jnp.log(jnp.sum(jnp.exp(every_mass - mass_peak[:, None]), axis=1))
    near_share = jnp.exp(near_mass - log_total)
    sent_row = jnp.any(slot_row[:, None, None] == own_place[None], axis=2)
    log_outgoing = jnp.where(
        jnp.any(sent_row, axis=1),
        jnp.sum(jnp.where(sent_row, log_total[None, :], 0.0), axis=1),
        absent_mass,
    )
    log_arrived = exchange(
        log_outgoing.reshape(device_count, slot_width), ("pb", "pa")
    ).reshape(plane_count, plane_rows)
    far_weight = []
    for order, (source, _) in enumerate(chunks):
        log_rows = chosen([log_arrived[p] for p in range(plane_count)], source)
        far_weight.append(
            jnp.exp(far_scores[order] - log_rows[:, None]).astype(jnp.bfloat16)
        )
    shifts = sorted(range(plane_count), key=lambda k: -min(k, plane_count - k))
    far_part = None
    for shift in shifts:
        goal = (plane + shift) % plane_count
        weight_rows = chosen(far_weight, chosen(orders, goal))
        share = jnp.dot(weight_rows, passages, preferred_element_type=jnp.float32)
        share = share.astype(jnp.bfloat16).reshape(column_count, slot_width, MODEL_WIDTH)
        share = exchange(share, "pa")
        merged = lax.dot_general(
            plane_hot(goal, None if shift else own_place).astype(jnp.bfloat16),
            share.reshape(plane_rows, MODEL_WIDTH),
            (((0,), (0,)), ((), ())),
            preferred_element_type=jnp.float32,
        )
        if shift:
            merged = lax.ppermute(
                merged.astype(jnp.bfloat16),
                "pb",
                [(i, (i + shift) % plane_count) for i in range(plane_count)],
            )
        far_part = merged.astype(jnp.float32) if far_part is None else far_part + merged.astype(jnp.float32)
    narrow_projection, hidden_state = layer_hidden(
        context, residual, whole_weight, adapter_down_weight, adapter_up_weight
    )
    positive_hot = positive[:, None] == jnp.arange(passage_count, dtype=jnp.int32)[None, :]
    positive_rows = jnp.dot(
        positive_hot.astype(jnp.bfloat16), passages, preferred_element_type=jnp.float32
    )
    own_part = near_share[:, None] * near_mean - positive_rows
    query_gradient = loss_scale * score_scale * (far_part + own_part)
    near_weight = (
        jnp.exp(near_scores - log_total[:, None]) - positive_hot.astype(jnp.float32)
    ).astype(jnp.bfloat16)
    product_dims = (((0,), (0,)), ((), ()))
    every_row = jnp.concatenate([queries] + arrived, axis=0)
    every_weight = jnp.concatenate([near_weight] + far_weight, axis=0)
    grad_passages = (loss_scale * score_scale) * lax.dot_general(
        every_weight, every_row, product_dims, preferred_element_type=jnp.float32
    )
    down_product, up_product = layer_parts(
        context,
        narrow_projection,
        hidden_state,
        adapter_up_weight,
        final_norm_weight,
        query_gradient[:RERUN_QUERIES],
    )
    rank = up_product.shape[0]
    adapter_terms = jnp.concatenate([down_product, up_product], axis=0)
    adapter_terms = adapter_terms.reshape(2 * rank, device_count, -1).transpose(1, 0, 2)
    adapter_sums = jnp.sum(
        exchange(adapter_terms.astype(jnp.bfloat16), ("pb", "pa")).astype(jnp.float32), axis=0
    )
    return (query_gradient, grad_passages, adapter_sums[:rank].T, adapter_sums[rank:])


def solution(mesh):
    placed = (
        P(("pb", "pa"), None),
        P(("pb", "pa"), None),
        P(("pb", "pa"), None),
        P(("pb", "pa")),
        P(("pb", "pa"), None),
        P(("pb", "pa"), None),
        P(("pb", "pa"), None),
        P(),
        P(),
        P(),
    )
    return jax.shard_map(
        local_step,
        mesh=mesh,
        in_specs=placed,
        out_specs=(
            P(("pb", "pa"), None),
            P(("pb", "pa"), None),
            P(("pb", "pa"), None),
            P(None, ("pb", "pa")),
        ),
        check_vma=False,
    )
```
